32 devices in a mesh: groups: 2 (over x), seq: 16 (over z, y, core).
Axes of the slice: x: 2, y: 2, z: 4, core: 2. Of those that a mesh axis runs over, the one named last changes fastest.
Arguments:
- hidden: bfloat16 [1024, 3072], P(('groups', 'seq')), parts along dimension 0, may hold values from -6 to 6
- queries: bfloat16 [1024, 3072], P(('groups', 'seq')), parts along dimension 0, may hold values from -6 to 6
- key_rows: bfloat16 [1024, 3072], P(('groups', 'seq')), parts along dimension 0, may hold values from -6 to 6
- values: bfloat16 [1024, 3072], P(('groups', 'seq')), parts along dimension 0, may hold values from -12 to 12
- query_gain: float32 [2, 128], replicated, may hold values from 0.6 to 5
- key_gain: float32 [2, 128], replicated, may hold values from 0.6 to 5
- gate_table: bfloat16 [8, 2, 3072], P('groups'), parts along dimension 0, may hold values from -6 to 6
- segment: int32 [1024], P(('groups', 'seq')), parts along dimension 0, may hold values from 0 to 3, as said below
- text_count: int32 [8], P('groups'), parts along dimension 0, may hold values from 1 to 40
Outputs:
- mixed: bfloat16 [1024, 3072], P(('groups', 'seq')), parts along dimension 0
The draws below stay inside these ranges and needn't reach their ends.
There are 2 independent parts, one for each index of `groups`. The reference program is written for one: setup_inputs(seed, part) draws one part's arguments, and reference() takes and returns one part's arrays. A program takes and returns all parts, laid end to end along the dimension named above; an argument that names none is the same for every part. Nothing has to cross between parts.
Inputs may be any that keep to these rules, and one draw needn't show every extreme that they name: `segment`: one device holds at most 10 tokens of one request; in every draw some two requests 2 j and 2 j + 1 get exactly 10 tokens from every device. Tokens of one request may lie anywhere on the devices.
All inputs are finite; a program needn't handle non-finite values.
Results may differ from the reference program's by a relative error of at most 0.012.
The reference program's roundings to bfloat16 on the way (of `query_normed`, `key_normed`, `weights` and `attention`) count: a program that leaves them out, or rounds other values in their place, can miss the bound.
Values may be sent and summed in bfloat16 or wider, within the bound.
A program may use at most 64 MiB of HBM per device.

```python
import math
import jax
import jax.numpy as jnp
from jax import lax

HEADS = 24
HEAD_DIM = 128
D = 3072
TOK_DEV = 32
TOKENS = 512
FINE = 4
CAP = 10
REQS = 4
N_SEQ = 16


def layout(key):
    base_key = jax.random.fold_in(key, 7)
    devices = TOKENS // TOK_DEV
    pair_key, seat_key, bias_key = jax.random.split(base_key, 3)
    full_pair = jax.random.randint(pair_key, (), 0, FINE // 2) * 2
    seat_count = FINE * CAP
    seat_slice = jnp.arange(seat_count, dtype=jnp.int32) // CAP
    forced = seat_slice // 2 * 2 == full_pair
    slice_bias = jax.random.randint(bias_key, (FINE,), 0, 1 << 15)

    def one_device(device_key):
        score_key, order_key = jax.random.split(device_key)
        seat_score = (jax.random.randint(score_key, (seat_count,), 0, 1 << 16) + slice_bias[seat_slice]) * seat_count + jnp.arange(seat_count, dtype=jnp.int32)
        seat_score = jnp.where(forced, -1 - jnp.arange(seat_count, dtype=jnp.int32), seat_score)
        chosen = jnp.argsort(seat_score)[:TOK_DEV]
        token_order = jax.random.permutation(order_key, TOK_DEV)
        return seat_slice[chosen][token_order]
    fine_slice = jax.vmap(one_device)(jax.random.split(seat_key, devices)).reshape(TOKENS)
    segment = fine_slice
    return segment


def drawn(key):
    own_key = jax.random.fold_in(key, 11)
    query_key, key_key = jax.random.split(own_key, 2)
    queries = jnp.clip(jax.random.normal(query_key, (TOKENS, D), jnp.float32), -6.0, 6.0)
    key_data = jnp.clip(jax.random.normal(key_key, (TOKENS, D), jnp.float32), -6.0, 6.0)
    return (queries, key_data)


def draw_segment(key, part):
    return layout(key).astype(jnp.int32)


def draw_queries(key, part):
    return drawn(key)[0].astype(jnp.bfloat16)


def draw_key_rows(key, part):
    return drawn(key)[1].astype(jnp.bfloat16)


def gain_draw(key):
    return jax.random.uniform(key, (2, HEAD_DIM), jnp.float32, 0.6, 1.6)


def draw_query_gain(key, part):
    return gain_draw(jax.random.fold_in(key, 21))


def draw_key_gain(key, part):
    return gain_draw(jax.random.fold_in(key, 23))


def with_ends(values, stream_key, smallest, high):
    longest = values.shape.index(max(values.shape))
    spots = []
    for shift in (0, 1):
        where = [jax.random.randint(jax.random.fold_in(stream_key, axis), (), 0, length) for axis, length in enumerate(values.shape)]
        where[longest] = (where[longest] + shift) % values.shape[longest]
        spots.append(tuple(where))
    return values.at[spots[0]].set(smallest).at[spots[1]].set(high)


def steps_of(stream_key, shape, shards, smallest, top_value):
    def one(dim, parts):
        heights = jax.random.uniform(jax.random.fold_in(jax.random.fold_in(stream_key, 6), dim), (parts,), jnp.float32, smallest / len(shards), top_value / len(shards))
        return jnp.repeat(jnp.exp(heights), shape[dim] // parts).reshape((-1,) + (1,) * (len(shape) - dim - 1))

    loudness = one(*shards[0])
    for cut in shards[1:]:
        loudness = loudness * one(*cut)
    return loudness


def centred(key, shape, deviation, reach, cuts=(), held_as=jnp.bfloat16):
    loudness = steps_of(key, shape, cuts, -0.22, 0.18) if cuts else 1.0
    array = jax.random.normal(key, shape, jnp.float32) * deviation * loudness
    return jnp.minimum(jnp.maximum(array, -reach), reach).astype(held_as)


def setup_inputs(seed: int = 0, part: int = 0) -> dict:
    key_list = jax.random.split(jax.random.key(seed), 10)
    own_keys = jax.random.split(jax.random.fold_in(key_list[9], part), 10)
    hidden = centred(own_keys[0], (TOKENS, D), 1.0, 6.0, ((0, 16),))
    queries = draw_queries(jax.random.fold_in(jax.random.fold_in(key_list[9], part), 71), part)
    key_rows = draw_key_rows(jax.random.fold_in(jax.random.fold_in(key_list[9], part), 71), part)
    values = centred(own_keys[3], (TOKENS, D), 2.0, 12.0, ((0, 16),))
    query_gain = draw_query_gain(jax.random.fold_in(key_list[9], 71), part)
    key_gain = draw_key_gain(jax.random.fold_in(key_list[9], 71), part)
    gate_table = centred(own_keys[6], (REQS, 2, D), 1.0, 6.0)
    segment = draw_segment(jax.random.fold_in(jax.random.fold_in(key_list[9], part), 71), part)
    text_count = with_ends(jax.random.randint(own_keys[8], (REQS,), 1, N_SEQ * CAP // 4 + 1), jax.random.fold_in(own_keys[8], 1), 1, (N_SEQ * CAP // 4 + 1) - 1).astype(jnp.int32)
    return dict(hidden=hidden, queries=queries, key_rows=key_rows, values=values, query_gain=query_gain, key_gain=key_gain, gate_table=gate_table, segment=segment, text_count=text_count)


EPSILON = 1e-06
MASKED = -1e+30

def head_norm(rows_in, gains, stream):
    row_count = rows_in.shape[0]
    per_head = rows_in.astype(jnp.float32).reshape(row_count, -1, HEAD_DIM)
    inverse = lax.rsqrt(lax.optimization_barrier(jnp.mean(per_head * per_head, axis=-1, keepdims=True)) + EPSILON)
    gain_rows = jnp.where((stream == 0)[:, None], gains[0][None, :], gains[1][None, :])
    return (per_head * inverse * gain_rows[:, None, :]).astype(jnp.bfloat16).reshape(row_count, -1)

def attend(query_block, block_segment, key_data, value_data, key_segment):
    scores = jnp.einsum('qhd,khd->hqk', query_block.astype(jnp.float32), key_data.astype(jnp.float32)) * (1.0 / math.sqrt(HEAD_DIM))
    allowed = (block_segment[:, None] == key_segment[None, :])[None, :, :]
    scores = jnp.where(allowed, scores, MASKED)
    largest = lax.optimization_barrier(jnp.max(scores, axis=-1, keepdims=True))
    weights = jnp.exp(scores - largest)
    weights = (weights / lax.optimization_barrier(jnp.sum(weights, axis=-1, keepdims=True))).astype(jnp.bfloat16)
    return jnp.einsum('hqk,khd->qhd', weights.astype(jnp.float32), value_data.astype(jnp.float32)).astype(jnp.bfloat16)

def reference(hidden, queries, key_rows, values, query_gain, key_gain, gate_table, segment, text_count):
    requests = text_count.shape[0]
    seg_hot = (segment[:, None] == jnp.arange(requests, dtype=jnp.int32)[None, :]).astype(jnp.int32)
    position = lax.optimization_barrier(jnp.sum((jnp.cumsum(seg_hot, axis=0) - seg_hot) * seg_hot, axis=1))
    text_limit = lax.optimization_barrier(jnp.sum(seg_hot * text_count[None, :], axis=1))
    stream = (position >= text_limit).astype(jnp.int32)
    query_normed = head_norm(queries, query_gain, stream)
    key_normed = head_norm(key_rows, key_gain, stream)
    fine_slice = segment.astype(jnp.int32)
    fine_hot = (fine_slice[:, None] == jnp.arange(FINE, dtype=jnp.int32)[None, :]).astype(jnp.int32)
    slice_rank = lax.optimization_barrier(jnp.sum((jnp.cumsum(fine_hot, axis=0) - fine_hot) * fine_hot, axis=1))
    slice_width = N_SEQ * CAP
    slot_table = jnp.full((FINE, slice_width), TOKENS, jnp.int32).at[fine_slice, slice_rank].set(jnp.arange(TOKENS, dtype=jnp.int32))
    zero_row = jnp.zeros((1, D), jnp.bfloat16)
    query_padded = jnp.concatenate([query_normed, zero_row], axis=0)
    key_padded = jnp.concatenate([key_normed, zero_row], axis=0)
    value_padded = jnp.concatenate([values, zero_row], axis=0)
    segment_padded = jnp.concatenate([segment, jnp.full((1,), -1, jnp.int32)], axis=0)

    def one_slice(slot_index):
        query_slice = jnp.take(query_padded, slot_index, axis=0).reshape(slice_width, HEADS, HEAD_DIM)
        key_slice = jnp.take(key_padded, slot_index, axis=0).reshape(slice_width, HEADS, HEAD_DIM)
        value_slice = jnp.take(value_padded, slot_index, axis=0).reshape(slice_width, HEADS, HEAD_DIM)
        slot_segment = jnp.take(segment_padded, slot_index, axis=0)
        result = attend(query_slice, slot_segment, key_slice, value_slice, slot_segment)
        return result.reshape(slice_width, D)
    blocks = lax.map(one_slice, slot_table)
    attention = jnp.zeros((TOKENS + 1, D), jnp.bfloat16).at[slot_table.reshape(-1)].set(blocks.reshape(-1, D))[:TOKENS]
    gate_rows = jnp.take(gate_table.reshape(requests * 2, D), segment * 2 + stream, axis=0)
    mixed = hidden.astype(jnp.float32) + gate_rows.astype(jnp.float32) * attention.astype(jnp.float32)
    return mixed.astype(jnp.bfloat16)
```

```python
import functools
import math

import jax
import jax.numpy as jnp
from jax import lax
from jax.experimental import pallas as pl
from jax.experimental.pallas import tpu as pltpu
from jax.sharding import PartitionSpec as P

HEAD_DIM = 128


EPSILON = 1e-06
MASKED = -1e30


def head_norm(rows_in, gains, stream):
    row_count = rows_in.shape[0]
    per_head = rows_in.astype(jnp.float32).reshape(row_count, -1, HEAD_DIM)
    inverse = lax.rsqrt(jnp.mean(per_head * per_head, axis=-1, keepdims=True) + EPSILON)
    gain_rows = jnp.where((stream == 0)[:, None], gains[0][None, :], gains[1][None, :])
    return (per_head * inverse * gain_rows[:, None, :]).astype(jnp.bfloat16).reshape(row_count, -1)


def attend(query_block, block_segment, key_data, value_data, key_segment):
    scores = jnp.einsum(
        "qhd,khd->hqk", query_block, key_data, preferred_element_type=jnp.float32
    ) * (1.0 / math.sqrt(HEAD_DIM))
    allowed = (block_segment[:, None] == key_segment[None, :])[None, :, :]
    scores = jnp.where(allowed, scores, MASKED)
    largest = jnp.max(scores, axis=-1, keepdims=True)
    weights = jnp.exp(scores - largest)
    weights = (weights / jnp.sum(weights, axis=-1, keepdims=True)).astype(jnp.bfloat16)
    return jnp.einsum(
        "hqk,khd->qhd", weights, value_data, preferred_element_type=jnp.float32
    ).astype(jnp.bfloat16)


def per_device(
    hidden, queries, key_rows, values, query_gain, key_gain, gate_table, segment, text_count
):
    tok_rows = hidden.shape[0]
    width_all = hidden.shape[1]
    devices = lax.axis_size("seq")
    requests = text_count.shape[0]
    seg_hot = (segment[:, None] == jnp.arange(requests, dtype=jnp.int32)[None, :]).astype(jnp.int32)
    local_counts = jnp.sum(seg_hot, axis=0)
    all_counts = lax.all_gather(local_counts[None, :], "seq", axis=0, tiled=True)
    lower_rows = (jnp.arange(devices, dtype=jnp.int32) < lax.axis_index("seq")).astype(jnp.int32)
    before = jnp.sum(all_counts * lower_rows[:, None], axis=0)
    position = jnp.sum((jnp.cumsum(seg_hot, axis=0) - seg_hot + before[None, :]) * seg_hot, axis=1)
    text_limit = jnp.sum(seg_hot * text_count[None, :], axis=1)
    stream = (position >= text_limit).astype(jnp.int32)
    query_normed = head_norm(queries, query_gain, stream)
    key_normed = head_norm(key_rows, key_gain, stream)
    groups = 8
    pair_merge = 2
    slices = devices // groups
    cap_rows = 4 * tok_rows // devices + max(1, tok_rows // devices)
    bucket_rows = cap_rows * pair_merge
    head_cols = width_all // groups
    owner_slice = segment // pair_merge
    owner_hot = (owner_slice[:, None] == jnp.arange(slices, dtype=jnp.int32)[None, :]).astype(
        jnp.int32
    )
    owner_rank = jnp.sum((jnp.cumsum(owner_hot, axis=0) - owner_hot) * owner_hot, axis=1)
    slot_place = owner_slice * bucket_rows + owner_rank
    bucket_index = (
        jnp.full((slices * bucket_rows,), tok_rows, jnp.int32)
        .at[slot_place]
        .set(jnp.arange(tok_rows, dtype=jnp.int32))
    )
    stacked = jnp.concatenate(
        [
            query_normed.reshape(tok_rows, groups, head_cols),
            key_normed.reshape(tok_rows, groups, head_cols),
            values.reshape(tok_rows, groups, head_cols),
        ],
        axis=2,
    ).transpose(1, 0, 2)
    outgoing = jnp.take(stacked, bucket_index, axis=1, mode="fill", fill_value=0).reshape(
        devices, bucket_rows, 3 * head_cols
    )
    slot_segment = jnp.take(segment, bucket_index, axis=0, mode="fill", fill_value=-1)
    segment_out = jnp.broadcast_to(slot_segment[None, :], (groups, slices * bucket_rows)).reshape(
        devices, bucket_rows
    )
    arrived, arrived_segment = (
        lax.all_to_all(outgoing, "seq", split_axis=0, concat_axis=0, tiled=True),
        lax.all_to_all(segment_out, "seq", split_axis=0, concat_axis=0, tiled=True),
    )
    slot_count = devices * bucket_rows
    per_head = head_cols // HEAD_DIM
    slot_data = arrived.reshape(slot_count, 3 * head_cols)
    query_all = slot_data[:, :head_cols].reshape(slot_count, per_head, HEAD_DIM)
    key_all = slot_data[:, head_cols : 2 * head_cols].reshape(slot_count, per_head, HEAD_DIM)
    value_all = slot_data[:, 2 * head_cols :].reshape(slot_count, per_head, HEAD_DIM)
    key_segment = arrived_segment.reshape(slot_count)
    if slot_count % 512 == 0:
        block_rows = 512
    elif slot_count % 256 == 0:
        block_rows = 256
    else:
        block_rows = slot_count

    def one_block(first_row):
        return attend(query_all, key_segment, key_all, value_all, key_segment)

    results = lax.map(one_block, jnp.arange(slot_count // block_rows, dtype=jnp.int32) * block_rows)
    returning = results.reshape(devices, bucket_rows, head_cols)
    returned = lax.all_to_all(returning, "seq", split_axis=0, concat_axis=0, tiled=True)
    returned = returned.reshape(groups, slices * bucket_rows, head_cols)
    attention = (
        jnp.take(returned, slot_place, axis=1).transpose(1, 0, 2).reshape(tok_rows, width_all)
    )
    gate_rows = jnp.take(gate_table.reshape(requests * 2, width_all), segment * 2 + stream, axis=0)
    mixed = hidden.astype(jnp.float32) + gate_rows.astype(jnp.float32) * attention.astype(
        jnp.float32
    )
    return mixed.astype(jnp.bfloat16)


LANES = 128
CONTRACT_LAST = (((1,), (1,)), ((), ()))


def normed(rows, gain_rows):
    wide = rows.astype(jnp.float32)
    inverse = lax.rsqrt(jnp.mean(wide * wide, axis=-1, keepdims=True) + EPSILON)
    return (wide * inverse * gain_rows).astype(jnp.bfloat16)


def fused_kernel(
    devices, requests, text_ref, segment_ref, hidden_ref, query_hbm, key_hbm, value_hbm,
    query_gain_ref, key_gain_ref, gate_ref, out_ref,
    stage, recv, query_n, key_n, result, back, seg_all, hot, text, bias, gate_rows,
    stage_sem, own_sem, seg_own_sem, seg_send, seg_recv,
    out_send, out_recv, relay_send, relay_recv, back_send, back_recv,
):
    chips = devices // 2
    tok = hidden_ref.shape[0]
    per_chip = hidden_ref.shape[1] // HEAD_DIM // chips
    tokens = devices * tok
    mine = chips * tok
    me = lax.axis_index("seq")
    chip, core = me // 2, me % 2
    partner = me + 1 - 2 * core
    sources = (query_hbm, key_hbm, value_hbm)

    def columns(head):
        return pl.ds(pl.multiple_of(head * HEAD_DIM, HEAD_DIM), HEAD_DIM)

    def remote(src, dst, send_sem, recv_sem, device):
        return pltpu.make_async_remote_copy(
            src_ref=src, dst_ref=dst, send_sem=send_sem, recv_sem=recv_sem,
            device_id={"seq": device}, device_id_type=pl.DeviceIdType.MESH,
        )

    barrier = pltpu.get_barrier_semaphore()
    for step in range(1, devices):
        pl.semaphore_signal(
            barrier, inc=1, device_id={"seq": (me + step) % devices},
            device_id_type=pl.DeviceIdType.MESH,
        )
    for head in range(per_chip):
        for step in range(1, chips):
            target = (chip + step) % chips
            for part, source in enumerate(sources):
                pltpu.make_async_copy(
                    source.at[:, columns(target * per_chip + head)],
                    stage.at[head, step - 1, part],
                    stage_sem.at[head],
                ).start()
        for part, source in enumerate(sources):
            pltpu.make_async_copy(
                source.at[:, columns(chip * per_chip + head)],
                recv.at[head, me, part],
                own_sem.at[head],
            ).start()
    seg_own = pltpu.make_async_copy(segment_ref, seg_all.at[me], seg_own_sem)
    seg_own.start()
    pl.semaphore_wait(barrier, devices - 1)

    seg_copies = []
    for step in range(1, devices):
        copy = remote(
            segment_ref, seg_all.at[me], seg_send.at[step - 1], seg_recv.at[step - 1],
            (me + step) % devices,
        )
        copy.start()
        seg_copies.append(copy)
    out_copies = []
    for head in range(per_chip):
        pltpu.make_async_copy(stage.at[head], stage.at[head], stage_sem.at[head]).wait()
        row = []
        for step in range(1, chips):
            copy = remote(
                stage.at[head, step - 1], recv.at[head, me],
                out_send.at[head, step - 1], out_recv.at[head, step - 1],
                (chip + step) % chips * 2 + core,
            )
            copy.start()
            row.append(copy)
        out_copies.append(row)

    relay_copies = []

    def relay(head, step, source):
        copy = remote(
            recv.at[head, source, pl.ds(1, 2)], recv.at[head, source, pl.ds(1, 2)],
            relay_send.at[head, step], relay_recv.at[head, step], partner,
        )
        copy.start()
        return copy

    for head in range(per_chip):
        pltpu.make_async_copy(
            recv.at[head, me], recv.at[head, me], own_sem.at[head]
        ).wait()
        relay_copies.append([relay(head, 0, me)])

    seg_own.wait()
    for copy in seg_copies:
        copy.wait_recv()
    eye = (
        lax.broadcasted_iota(jnp.int32, (tok, tok), 0)
        == lax.broadcasted_iota(jnp.int32, (tok, tok), 1)
    ).astype(jnp.float32).astype(jnp.bfloat16)
    ids = lax.broadcasted_iota(jnp.int32, (LANES, tok), 0)
    for n in range(devices):
        flipped = (ids == seg_all[n]).astype(jnp.float32).astype(jnp.bfloat16)
        hot[n] = lax.dot_general(
            eye, flipped, CONTRACT_LAST, preferred_element_type=jnp.float32
        ).astype(jnp.bfloat16)
    all_hot = hot[...].reshape(tokens, LANES)
    earlier = (
        lax.broadcasted_iota(jnp.int32, (tokens, tokens), 1)
        < lax.broadcasted_iota(jnp.int32, (tokens, tokens), 0)
    ).astype(jnp.float32).astype(jnp.bfloat16)
    before = jnp.dot(earlier, all_hot, preferred_element_type=jnp.float32)
    lane = lax.broadcasted_iota(jnp.int32, (1, LANES), 1)
    limit = jnp.zeros((1, LANES), jnp.int32)
    for r in range(requests):
        limit = jnp.where(lane == r, text_ref[r], limit)
    inside = jnp.where(before < limit.astype(jnp.float32), all_hot.astype(jnp.float32), 0.0)
    ones = jnp.ones((LANES, LANES), jnp.bfloat16)
    text[...] = jnp.dot(
        inside.astype(jnp.bfloat16), ones, preferred_element_type=jnp.float32
    ).reshape(devices, tok, LANES)
    for c in range(chips):
        same = lax.dot_general(
            hot[2 * c + core], all_hot, CONTRACT_LAST, preferred_element_type=jnp.float32
        )
        bias[c * tok : (c + 1) * tok] = jnp.where(same > 0.5, 0.0, MASKED)

    number = lax.broadcasted_iota(jnp.int32, (LANES, LANES), 0).astype(jnp.float32)
    own_id = jnp.dot(
        hot[me], number.astype(jnp.bfloat16), preferred_element_type=jnp.float32
    )
    own_code = 2.0 * own_id + jnp.where(text[me] > 0.5, 0.0, 1.0)
    for tile in range(hidden_ref.shape[1] // LANES):
        cols = slice(tile * LANES, (tile + 1) * LANES)
        total = jnp.zeros((tok, LANES), jnp.float32)
        for r in range(requests):
            pair = gate_ref[r, :, cols].astype(jnp.float32)
            for s in range(2):
                total = jnp.where(own_code == float(2 * r + s), pair[s : s + 1], total)
        gate_rows[tile] = total

    query_gain, key_gain = query_gain_ref[...], key_gain_ref[...]

    def gain_of(gain, n):
        return jnp.where(text[n] > 0.5, gain[0:1], gain[1:2])

    scale = 1.0 / math.sqrt(HEAD_DIM)
    back_copies = []
    for head in range(per_chip):
        for step in range(1, chips):
            out_copies[head][step - 1].wait_recv()
            source = (chip + chips - step) % chips * 2 + core
            relay_copies[head].append(relay(head, step, source))
        for c in range(chips):
            n = 2 * c + core
            query_n[c] = normed(recv[head, n, 0], gain_of(query_gain, n))
            key_n[n] = normed(recv[head, n, 1], gain_of(key_gain, n))
        for step in range(chips):
            relay_copies[head][step].wait_recv()
            n = (chip + chips - step) % chips * 2 + 1 - core
            key_n[n] = normed(recv[head, n, 1], gain_of(key_gain, n))
        keys = key_n[...].reshape(tokens, HEAD_DIM)
        vals = recv[head, :, 2].reshape(tokens, HEAD_DIM)
        scores = lax.dot_general(
            query_n[...].reshape(mine, HEAD_DIM), keys, CONTRACT_LAST,
            preferred_element_type=jnp.float32,
        ) * scale + bias[...]
        largest = jnp.max(scores, axis=-1, keepdims=True)
        weights = jnp.exp(scores - largest)
        weights = (weights / jnp.sum(weights, axis=-1, keepdims=True)).astype(jnp.bfloat16)
        result[head] = jnp.dot(
            weights, vals, preferred_element_type=jnp.float32
        ).astype(jnp.bfloat16).reshape(chips, tok, HEAD_DIM)
        row = []
        for step in range(1, chips):
            target = (chip + step) % chips
            copy = remote(
                result.at[head, target], back.at[chip * per_chip + head],
                back_send.at[head, step - 1], back_recv.at[head, step - 1],
                target * 2 + core,
            )
            copy.start()
            row.append(copy)
        back_copies.append(row)

    def finish(index, attention):
        out_ref[:, columns(index)] = (
            hidden_ref[:, columns(index)].astype(jnp.float32)
            + gate_rows[index] * attention.astype(jnp.float32)
        ).astype(jnp.bfloat16)

    for head in range(per_chip):
        finish(chip * per_chip + head, result[head, chip])
        for step in range(1, chips):
            back_copies[head][step - 1].wait_recv()
            index = (chip + chips - step) % chips * per_chip + head
            finish(index, back[index])
    for copy in seg_copies:
        copy.wait_send()
    for rows in (out_copies, relay_copies, back_copies):
        for row in rows:
            for copy in row:
                copy.wait_send()


def fused(
    hidden, queries, key_rows, values, query_gain, key_gain, gate_table, segment, text_count
):
    devices = lax.axis_size("seq")
    chips = devices // 2
    tok, width = hidden.shape
    heads = width // HEAD_DIM
    per_chip = heads // chips
    vmem = pl.BlockSpec(memory_space=pltpu.VMEM)
    hbm = pl.BlockSpec(memory_space=pl.ANY)
    block = (tok, HEAD_DIM)
    dma = pltpu.SemaphoreType.DMA
    return pl.pallas_call(
        functools.partial(fused_kernel, devices, text_count.shape[0]),
        out_shape=jax.ShapeDtypeStruct((tok, width), jnp.bfloat16),
        in_specs=[pl.BlockSpec(memory_space=pltpu.SMEM), vmem, vmem, hbm, hbm, hbm]
        + [vmem] * 3,
        out_specs=vmem,
        scratch_shapes=[
            pltpu.VMEM((per_chip, chips - 1, 3) + block, jnp.bfloat16),
            pltpu.VMEM((per_chip, devices, 3) + block, jnp.bfloat16),
            pltpu.VMEM((chips,) + block, jnp.bfloat16),
            pltpu.VMEM((devices,) + block, jnp.bfloat16),
            pltpu.VMEM((per_chip, chips) + block, jnp.bfloat16),
            pltpu.VMEM((heads,) + block, jnp.bfloat16),
            pltpu.VMEM((devices, 1, tok), jnp.int32),
            pltpu.VMEM((devices, tok, LANES), jnp.bfloat16),
            pltpu.VMEM((devices, tok, LANES), jnp.float32),
            pltpu.VMEM((chips * tok, devices * tok), jnp.float32),
            pltpu.VMEM((heads, tok, LANES), jnp.float32),
            dma((per_chip,)),
            dma((per_chip,)),
            dma,
            dma((devices - 1,)),
            dma((devices - 1,)),
            dma((per_chip, chips - 1)),
            dma((per_chip, chips - 1)),
            dma((per_chip, chips)),
            dma((per_chip, chips)),
            dma((per_chip, chips - 1)),
            dma((per_chip, chips - 1)),
        ],
        compiler_params=pltpu.CompilerParams(collective_id=0, has_side_effects=True),
    )(
        text_count, segment.reshape(1, tok), hidden, queries, key_rows, values,
        query_gain, key_gain, gate_table,
    )


def program(*arrays):
    devices = lax.axis_size("seq")
    tok, width = arrays[0].shape
    requests = arrays[-1].shape[0]
    whole_heads = devices % 2 == 0 and (width // HEAD_DIM) % (devices // 2) == 0
    if whole_heads and devices * tok <= 1024 and requests <= LANES and tok % 16 == 0:
        return fused(*arrays)
    return per_device(*arrays)


def solution(mesh):
    return jax.shard_map(
        program,
        mesh=mesh,
        in_specs=(
            P(("groups", "seq"), None),
            P(("groups", "seq"), None),
            P(("groups", "seq"), None),
            P(("groups", "seq"), None),
            P(),
            P(),
            P("groups", None, None),
            P(("groups", "seq")),
            P("groups"),
        ),
        out_specs=P(("groups", "seq"), None),
        check_vma=False,
    )
```

```python
import functools
import math

import jax
import jax.numpy as jnp
from jax import lax
from jax.experimental import pallas as pl
from jax.experimental.pallas import tpu as pltpu
from jax.sharding import PartitionSpec as P

HEAD_DIM = 128


EPSILON = 1e-06
MASKED = -1e30


def head_norm(rows_in, gains, stream):
    row_count = rows_in.shape[0]
    per_head = rows_in.astype(jnp.float32).reshape(row_count, -1, HEAD_DIM)
    inverse = lax.rsqrt(jnp.mean(per_head * per_head, axis=-1, keepdims=True) + EPSILON)
    gain_rows = jnp.where((stream == 0)[:, None], gains[0][None, :], gains[1][None, :])
    return (per_head * inverse * gain_rows[:, None, :]).astype(jnp.bfloat16).reshape(row_count, -1)


def attend(query_block, block_segment, key_data, value_data, key_segment):
    scores = jnp.einsum(
        "qhd,khd->hqk", query_block, key_data, preferred_element_type=jnp.float32
    ) * (1.0 / math.sqrt(HEAD_DIM))
    allowed = (block_segment[:, None] == key_segment[None, :])[None, :, :]
    scores = jnp.where(allowed, scores, MASKED)
    largest = jnp.max(scores, axis=-1, keepdims=True)
    weights = jnp.exp(scores - largest)
    weights = (weights / jnp.sum(weights, axis=-1, keepdims=True)).astype(jnp.bfloat16)
    return jnp.einsum(
        "hqk,khd->qhd", weights, value_data, preferred_element_type=jnp.float32
    ).astype(jnp.bfloat16)


def per_device(
    hidden, queries, key_rows, values, query_gain, key_gain, gate_table, segment, text_count
):
    tok_rows = hidden.shape[0]
    width_all = hidden.shape[1]
    devices = lax.axis_size("seq")
    requests = text_count.shape[0]
    seg_hot = (segment[:, None] == jnp.arange(requests, dtype=jnp.int32)[None, :]).astype(jnp.int32)
    local_counts = jnp.sum(seg_hot, axis=0)
    all_counts = lax.all_gather(local_counts[None, :], "seq", axis=0, tiled=True)
    lower_rows = (jnp.arange(devices, dtype=jnp.int32) < lax.axis_index("seq")).astype(jnp.int32)
    before = jnp.sum(all_counts * lower_rows[:, None], axis=0)
    position = jnp.sum((jnp.cumsum(seg_hot, axis=0) - seg_hot + before[None, :]) * seg_hot, axis=1)
    text_limit = jnp.sum(seg_hot * text_count[None, :], axis=1)
    stream = (position >= text_limit).astype(jnp.int32)
    query_normed = head_norm(queries, query_gain, stream)
    key_normed = head_norm(key_rows, key_gain, stream)
    groups = 8
    pair_merge = 2
    slices = devices // groups
    cap_rows = 4 * tok_rows // devices + max(1, tok_rows // devices)
    bucket_rows = cap_rows * pair_merge
    head_cols = width_all // groups
    owner_slice = segment // pair_merge
    owner_hot = (owner_slice[:, None] == jnp.arange(slices, dtype=jnp.int32)[None, :]).astype(
        jnp.int32
    )
    owner_rank = jnp.sum((jnp.cumsum(owner_hot, axis=0) - owner_hot) * owner_hot, axis=1)
    slot_place = owner_slice * bucket_rows + owner_rank
    bucket_index = (
        jnp.full((slices * bucket_rows,), tok_rows, jnp.int32)
        .at[slot_place]
        .set(jnp.arange(tok_rows, dtype=jnp.int32))
    )
    stacked = jnp.concatenate(
        [
            query_normed.reshape(tok_rows, groups, head_cols),
            key_normed.reshape(tok_rows, groups, head_cols),
            values.reshape(tok_rows, groups, head_cols),
        ],
        axis=2,
    ).transpose(1, 0, 2)
    outgoing = jnp.take(stacked, bucket_index, axis=1, mode="fill", fill_value=0).reshape(
        devices, bucket_rows, 3 * head_cols
    )
    slot_segment = jnp.take(segment, bucket_index, axis=0, mode="fill", fill_value=-1)
    segment_out = jnp.broadcast_to(slot_segment[None, :], (groups, slices * bucket_rows)).reshape(
        devices, bucket_rows
    )
    arrived, arrived_segment = (
        lax.all_to_all(outgoing, "seq", split_axis=0, concat_axis=0, tiled=True),
        lax.all_to_all(segment_out, "seq", split_axis=0, concat_axis=0, tiled=True),
    )
    slot_count = devices * bucket_rows
    per_head = head_cols // HEAD_DIM
    slot_data = arrived.reshape(slot_count, 3 * head_cols)
    query_all = slot_data[:, :head_cols].reshape(slot_count, per_head, HEAD_DIM)
    key_all = slot_data[:, head_cols : 2 * head_cols].reshape(slot_count, per_head, HEAD_DIM)
    value_all = slot_data[:, 2 * head_cols :].reshape(slot_count, per_head, HEAD_DIM)
    key_segment = arrived_segment.reshape(slot_count)
    if slot_count % 512 == 0:
        block_rows = 512
    elif slot_count % 256 == 0:
        block_rows = 256
    else:
        block_rows = slot_count

    def one_block(first_row):
        return attend(query_all, key_segment, key_all, value_all, key_segment)

    results = lax.map(one_block, jnp.arange(slot_count // block_rows, dtype=jnp.int32) * block_rows)
    returning = results.reshape(devices, bucket_rows, head_cols)
    returned = lax.all_to_all(returning, "seq", split_axis=0, concat_axis=0, tiled=True)
    returned = returned.reshape(groups, slices * bucket_rows, head_cols)
    attention = (
        jnp.take(returned, slot_place, axis=1).transpose(1, 0, 2).reshape(tok_rows, width_all)
    )
    gate_rows = jnp.take(gate_table.reshape(requests * 2, width_all), segment * 2 + stream, axis=0)
    mixed = hidden.astype(jnp.float32) + gate_rows.astype(jnp.float32) * attention.astype(
        jnp.float32
    )
    return mixed.astype(jnp.bfloat16)


LANES = 128
CONTRACT_LAST = (((1,), (1,)), ((), ()))


def normed(rows, gain_rows):
    wide = rows.astype(jnp.float32)
    inverse = lax.rsqrt(jnp.mean(wide * wide, axis=-1, keepdims=True) + EPSILON)
    return (wide * inverse * gain_rows).astype(jnp.bfloat16)


def fused_kernel(
    devices, requests, segment_hbm, query_hbm, key_hbm, value_hbm,
    text_hbm, hidden_hbm, query_gain_hbm, key_gain_hbm, gate_hbm, out_hbm,
    text_ref, hidden_ref, query_gain_ref, key_gain_ref, gate_ref, out_ref,
    stage, recv, query_n, key_n, result, back, seg_all, hot, text, bias, gate_rows,
    stage_sem, own_sem, seg_own_sem, load_sem, store_sem, seg_send, seg_recv,
    out_send, out_recv, relay_send, relay_recv, back_send, back_recv,
):
    chips = devices // 2
    tok = hidden_hbm.shape[0]
    per_chip = hidden_hbm.shape[1] // HEAD_DIM // chips
    tokens = devices * tok
    mine = chips * tok
    me = lax.axis_index("seq")
    chip, core = me // 2, me % 2
    partner = me + 1 - 2 * core
    sources = (query_hbm, key_hbm, value_hbm)

    def columns(head):
        return pl.ds(pl.multiple_of(head * HEAD_DIM, HEAD_DIM), HEAD_DIM)

    def remote(src, dst, send_sem, recv_sem, device):
        return pltpu.make_async_remote_copy(
            src_ref=src, dst_ref=dst, send_sem=send_sem, recv_sem=recv_sem,
            device_id={"seq": device}, device_id_type=pl.DeviceIdType.MESH,
        )

    barrier = pltpu.get_barrier_semaphore()
    for device in [(chip + step) % chips * 2 + core for step in range(1, chips)] + [partner]:
        pl.semaphore_signal(
            barrier, inc=1, device_id={"seq": device},
            device_id_type=pl.DeviceIdType.MESH,
        )
    seg_own = pltpu.make_async_copy(segment_hbm, seg_all.at[me], seg_own_sem)
    seg_own.start()
    for head in range(per_chip):
        for step in range(1, chips):
            target = (chip + step) % chips
            for part, source in enumerate(sources):
                pltpu.make_async_copy(
                    source.at[:, columns(target * per_chip + head)],
                    stage.at[head, step - 1, part],
                    stage_sem.at[head],
                ).start()
        for part, source in enumerate(sources):
            pltpu.make_async_copy(
                source.at[:, columns(chip * per_chip + head)],
                recv.at[head, me, part],
                own_sem.at[head],
            ).start()
    loads = [
        pltpu.make_async_copy(source, target, load_sem.at[place])
        for place, (source, target) in enumerate(
            (
                (text_hbm, text_ref), (query_gain_hbm, query_gain_ref),
                (key_gain_hbm, key_gain_ref), (gate_hbm, gate_ref), (hidden_hbm, hidden_ref),
            )
        )
    ]
    for copy in loads:
        copy.start()
    seg_own.wait()
    pl.semaphore_wait(barrier, chips)

    seg_copies = []
    seg_relays = []

    def send_ids(source, kind, step, device):
        copy = remote(
            seg_all.at[source], seg_all.at[source],
            seg_send.at[kind, step], seg_recv.at[kind, step], device,
        )
        copy.start()
        return copy

    for step in range(chips - 1, 0, -1):
        seg_copies.insert(0, send_ids(me, 0, step, (chip + step) % chips * 2 + core))
    seg_relays.append(send_ids(me, 1, 0, partner))
    out_copies = []
    for head in range(per_chip):
        pltpu.make_async_copy(stage.at[head], stage.at[head], stage_sem.at[head]).wait()
        row = []
        for step in range(chips - 1, 0, -1):
            copy = remote(
                stage.at[head, step - 1], recv.at[head, me],
                out_send.at[head, step - 1], out_recv.at[head, step - 1],
                (chip + step) % chips * 2 + core,
            )
            copy.start()
            row.insert(0, copy)
        out_copies.append(row)

    relay_copies = []

    def relay(head, step, source):
        copy = remote(
            recv.at[head, source, pl.ds(1, 2)], recv.at[head, source, pl.ds(1, 2)],
            relay_send.at[head, step], relay_recv.at[head, step], partner,
        )
        copy.start()
        return copy

    for head in range(per_chip):
        pltpu.make_async_copy(
            recv.at[head, me], recv.at[head, me], own_sem.at[head]
        ).wait()
        relay_copies.append([relay(head, 0, me)])

    for step in range(1, chips):
        seg_copies[step - 1].wait_recv()
        source = (chip + chips - step) % chips * 2 + core
        seg_relays.append(send_ids(source, 1, step, partner))
    for copy in seg_relays:
        copy.wait_recv()
    for copy in loads:
        copy.wait()
    eye = (
        lax.broadcasted_iota(jnp.int32, (tok, tok), 0)
        == lax.broadcasted_iota(jnp.int32, (tok, tok), 1)
    ).astype(jnp.float32).astype(jnp.bfloat16)
    ids = lax.broadcasted_iota(jnp.int32, (LANES, tok), 0)
    for n in range(devices):
        flipped = (ids == seg_all[n]).astype(jnp.float32).astype(jnp.bfloat16)
        hot[n] = lax.dot_general(
            eye, flipped, CONTRACT_LAST, preferred_element_type=jnp.float32
        ).astype(jnp.bfloat16)
    all_hot = hot[...].reshape(tokens, LANES)
    earlier = (
        lax.broadcasted_iota(jnp.int32, (tokens, tokens), 1)
        < lax.broadcasted_iota(jnp.int32, (tokens, tokens), 0)
    ).astype(jnp.float32).astype(jnp.bfloat16)
    before = jnp.dot(earlier, all_hot, preferred_element_type=jnp.float32)
    lane = lax.broadcasted_iota(jnp.int32, (1, LANES), 1)
    limit = jnp.zeros((1, LANES), jnp.int32)
    for r in range(requests):
        limit = jnp.where(lane == r, text_ref[0:1, r : r + 1], limit)
    inside = jnp.where(before < limit.astype(jnp.float32), all_hot.astype(jnp.float32), 0.0)
    ones = jnp.ones((LANES, LANES), jnp.bfloat16)
    text[...] = jnp.dot(
        inside.astype(jnp.bfloat16), ones, preferred_element_type=jnp.float32
    ).reshape(devices, tok, LANES)
    for c in range(chips):
        same = lax.dot_general(
            hot[2 * c + core], all_hot, CONTRACT_LAST, preferred_element_type=jnp.float32
        )
        bias[c * tok : (c + 1) * tok] = jnp.where(same > 0.5, 0.0, MASKED)

    number = lax.broadcasted_iota(jnp.int32, (LANES, LANES), 0).astype(jnp.float32)
    own_id = jnp.dot(
        hot[me], number.astype(jnp.bfloat16), preferred_element_type=jnp.float32
    )
    own_code = 2.0 * own_id + jnp.where(text[me] > 0.5, 0.0, 1.0)
    for tile in range(hidden_ref.shape[1] // LANES):
        cols = slice(tile * LANES, (tile + 1) * LANES)
        total = jnp.zeros((tok, LANES), jnp.float32)
        for r in range(requests):
            pair = gate_ref[r, :, cols].astype(jnp.float32)
            for s in range(2):
                total = jnp.where(own_code == float(2 * r + s), pair[s : s + 1], total)
        gate_rows[tile] = total

    query_gain, key_gain = query_gain_ref[...], key_gain_ref[...]

    def gain_of(gain, n):
        return jnp.where(text[n] > 0.5, gain[0:1], gain[1:2])

    scale = 1.0 / math.sqrt(HEAD_DIM)
    back_copies = []
    for head in range(per_chip):
        for step in range(1, chips):
            out_copies[head][step - 1].wait_recv()
            source = (chip + chips - step) % chips * 2 + core
            relay_copies[head].append(relay(head, step, source))
        for c in range(chips):
            n = 2 * c + core
            query_n[c] = normed(recv[head, n, 0], gain_of(query_gain, n))
            key_n[n] = normed(recv[head, n, 1], gain_of(key_gain, n))
        for step in range(chips):
            relay_copies[head][step].wait_recv()
            n = (chip + chips - step) % chips * 2 + 1 - core
            key_n[n] = normed(recv[head, n, 1], gain_of(key_gain, n))
        keys = key_n[...].reshape(tokens, HEAD_DIM)
        vals = recv[head, :, 2].reshape(tokens, HEAD_DIM)
        scores = lax.dot_general(
            query_n[...].reshape(mine, HEAD_DIM), keys, CONTRACT_LAST,
            preferred_element_type=jnp.float32,
        ) * scale + bias[...]
        largest = jnp.max(scores, axis=-1, keepdims=True)
        weights = jnp.exp(scores - largest)
        weights = (weights / jnp.sum(weights, axis=-1, keepdims=True)).astype(jnp.bfloat16)
        result[head] = jnp.dot(
            weights, vals, preferred_element_type=jnp.float32
        ).astype(jnp.bfloat16).reshape(chips, tok, HEAD_DIM)
        row = []
        for step in range(1, chips):
            target = (chip + step) % chips
            copy = remote(
                result.at[head, target], back.at[chip * per_chip + head],
                back_send.at[head, step - 1], back_recv.at[head, step - 1],
                target * 2 + core,
            )
            copy.start()
            row.append(copy)
        back_copies.append(row)

    def finish(index, attention):
        out_ref[:, columns(index)] = (
            hidden_ref[:, columns(index)].astype(jnp.float32)
            + gate_rows[index] * attention.astype(jnp.float32)
        ).astype(jnp.bfloat16)
        pltpu.make_async_copy(
            out_ref.at[:, columns(index)], out_hbm.at[:, columns(index)], store_sem
        ).start()

    for head in range(per_chip):
        finish(chip * per_chip + head, result[head, chip])
        for step in range(1, chips):
            back_copies[head][step - 1].wait_recv()
            index = (chip + chips - step) % chips * per_chip + head
            finish(index, back[index])
    for copy in seg_copies + seg_relays:
        copy.wait_send()
    for rows in (out_copies, relay_copies, back_copies):
        for row in rows:
            for copy in row:
                copy.wait_send()
    pltpu.make_async_copy(out_ref, out_hbm, store_sem).wait()


def fused(
    hidden, queries, key_rows, values, query_gain, key_gain, gate_table, segment, text_count
):
    devices = lax.axis_size("seq")
    chips = devices // 2
    tok, width = hidden.shape
    heads = width // HEAD_DIM
    per_chip = heads // chips
    hbm = pl.BlockSpec(memory_space=pl.ANY)
    block = (tok, HEAD_DIM)
    dma = pltpu.SemaphoreType.DMA
    return pl.pallas_call(
        functools.partial(fused_kernel, devices, text_count.shape[0]),
        out_shape=jax.ShapeDtypeStruct((tok, width), jnp.bfloat16),
        in_specs=[hbm] * 9,
        out_specs=hbm,
        scratch_shapes=[
            pltpu.VMEM((1, text_count.shape[0]), jnp.int32),
            pltpu.VMEM(hidden.shape, hidden.dtype),
            pltpu.VMEM(query_gain.shape, query_gain.dtype),
            pltpu.VMEM(key_gain.shape, key_gain.dtype),
            pltpu.VMEM(gate_table.shape, gate_table.dtype),
            pltpu.VMEM(hidden.shape, jnp.bfloat16),
            pltpu.VMEM((per_chip, chips - 1, 3) + block, jnp.bfloat16),
            pltpu.VMEM((per_chip, devices, 3) + block, jnp.bfloat16),
            pltpu.VMEM((chips,) + block, jnp.bfloat16),
            pltpu.VMEM((devices,) + block, jnp.bfloat16),
            pltpu.VMEM((per_chip, chips) + block, jnp.bfloat16),
            pltpu.VMEM((heads,) + block, jnp.bfloat16),
            pltpu.VMEM((devices, 1, tok), jnp.int32),
            pltpu.VMEM((devices, tok, LANES), jnp.bfloat16),
            pltpu.VMEM((devices, tok, LANES), jnp.float32),
            pltpu.VMEM((chips * tok, devices * tok), jnp.float32),
            pltpu.VMEM((heads, tok, LANES), jnp.float32),
            dma((per_chip,)),
            dma((per_chip,)),
            dma,
            dma((5,)),
            dma,
            dma((2, chips)),
            dma((2, chips)),
            dma((per_chip, chips - 1)),
            dma((per_chip, chips - 1)),
            dma((per_chip, chips)),
            dma((per_chip, chips)),
            dma((per_chip, chips - 1)),
            dma((per_chip, chips - 1)),
        ],
        compiler_params=pltpu.CompilerParams(collective_id=0, has_side_effects=True),
    )(
        segment.reshape(1, tok), queries, key_rows, values,
        text_count.reshape(1, -1), hidden, query_gain, key_gain, gate_table,
    )


def program(*arrays):
    devices = lax.axis_size("seq")
    tok, width = arrays[0].shape
    requests = arrays[-1].shape[0]
    whole_heads = devices % 2 == 0 and (width // HEAD_DIM) % (devices // 2) == 0
    if whole_heads and devices * tok <= 1024 and requests <= LANES and tok % 16 == 0:
        return fused(*arrays)
    return per_device(*arrays)


def solution(mesh):
    return jax.shard_map(
        program,
        mesh=mesh,
        in_specs=(
            P(("groups", "seq"), None),
            P(("groups", "seq"), None),
            P(("groups", "seq"), None),
            P(("groups", "seq"), None),
            P(),
            P(),
            P("groups", None, None),
            P(("groups", "seq")),
            P("groups"),
        ),
        out_specs=P(("groups", "seq"), None),
        check_vma=False,
    )
```

```python
import functools
import math

import jax
import jax.numpy as jnp
from jax import lax
from jax.experimental import pallas as pl
from jax.experimental.pallas import tpu as pltpu
from jax.sharding import PartitionSpec as P

HEAD_DIM = 128


EPSILON = 1e-06
MASKED = -1e30


def head_norm(rows_in, gains, stream):
    row_count = rows_in.shape[0]
    per_head = rows_in.astype(jnp.float32).reshape(row_count, -1, HEAD_DIM)
    inverse = lax.rsqrt(jnp.mean(per_head * per_head, axis=-1, keepdims=True) + EPSILON)
    gain_rows = jnp.where((stream == 0)[:, None], gains[0][None, :], gains[1][None, :])
    return (per_head * inverse * gain_rows[:, None, :]).astype(jnp.bfloat16).reshape(row_count, -1)


def attend(query_block, block_segment, key_data, value_data, key_segment):
    scores = jnp.einsum(
        "qhd,khd->hqk", query_block, key_data, preferred_element_type=jnp.float32
    ) * (1.0 / math.sqrt(HEAD_DIM))
    allowed = (block_segment[:, None] == key_segment[None, :])[None, :, :]
    scores = jnp.where(allowed, scores, MASKED)
    largest = jnp.max(scores, axis=-1, keepdims=True)
    weights = jnp.exp(scores - largest)
    weights = (weights / jnp.sum(weights, axis=-1, keepdims=True)).astype(jnp.bfloat16)
    return jnp.einsum(
        "hqk,khd->qhd", weights, value_data, preferred_element_type=jnp.float32
    ).astype(jnp.bfloat16)


def per_device(
    hidden, queries, key_rows, values, query_gain, key_gain, gate_table, segment, text_count
):
    tok_rows = hidden.shape[0]
    width_all = hidden.shape[1]
    devices = lax.axis_size("seq")
    requests = text_count.shape[0]
    seg_hot = (segment[:, None] == jnp.arange(requests, dtype=jnp.int32)[None, :]).astype(jnp.int32)
    local_counts = jnp.sum(seg_hot, axis=0)
    all_counts = lax.all_gather(local_counts[None, :], "seq", axis=0, tiled=True)
    lower_rows = (jnp.arange(devices, dtype=jnp.int32) < lax.axis_index("seq")).astype(jnp.int32)
    before = jnp.sum(all_counts * lower_rows[:, None], axis=0)
    position = jnp.sum((jnp.cumsum(seg_hot, axis=0) - seg_hot + before[None, :]) * seg_hot, axis=1)
    text_limit = jnp.sum(seg_hot * text_count[None, :], axis=1)
    stream = (position >= text_limit).astype(jnp.int32)
    query_normed = head_norm(queries, query_gain, stream)
    key_normed = head_norm(key_rows, key_gain, stream)
    groups = 8
    pair_merge = 2
    slices = devices // groups
    cap_rows = 4 * tok_rows // devices + max(1, tok_rows // devices)
    bucket_rows = cap_rows * pair_merge
    head_cols = width_all // groups
    owner_slice = segment // pair_merge
    owner_hot = (owner_slice[:, None] == jnp.arange(slices, dtype=jnp.int32)[None, :]).astype(
        jnp.int32
    )
    owner_rank = jnp.sum((jnp.cumsum(owner_hot, axis=0) - owner_hot) * owner_hot, axis=1)
    slot_place = owner_slice * bucket_rows + owner_rank
    bucket_index = (
        jnp.full((slices * bucket_rows,), tok_rows, jnp.int32)
        .at[slot_place]
        .set(jnp.arange(tok_rows, dtype=jnp.int32))
    )
    stacked = jnp.concatenate(
        [
            query_normed.reshape(tok_rows, groups, head_cols),
            key_normed.reshape(tok_rows, groups, head_cols),
            values.reshape(tok_rows, groups, head_cols),
        ],
        axis=2,
    ).transpose(1, 0, 2)
    outgoing = jnp.take(stacked, bucket_index, axis=1, mode="fill", fill_value=0).reshape(
        devices, bucket_rows, 3 * head_cols
    )
    slot_segment = jnp.take(segment, bucket_index, axis=0, mode="fill", fill_value=-1)
    segment_out = jnp.broadcast_to(slot_segment[None, :], (groups, slices * bucket_rows)).reshape(
        devices, bucket_rows
    )
    arrived, arrived_segment = (
        lax.all_to_all(outgoing, "seq", split_axis=0, concat_axis=0, tiled=True),
        lax.all_to_all(segment_out, "seq", split_axis=0, concat_axis=0, tiled=True),
    )
    slot_count = devices * bucket_rows
    per_head = head_cols // HEAD_DIM
    slot_data = arrived.reshape(slot_count, 3 * head_cols)
    query_all = slot_data[:, :head_cols].reshape(slot_count, per_head, HEAD_DIM)
    key_all = slot_data[:, head_cols : 2 * head_cols].reshape(slot_count, per_head, HEAD_DIM)
    value_all = slot_data[:, 2 * head_cols :].reshape(slot_count, per_head, HEAD_DIM)
    key_segment = arrived_segment.reshape(slot_count)
    if slot_count % 512 == 0:
        block_rows = 512
    elif slot_count % 256 == 0:
        block_rows = 256
    else:
        block_rows = slot_count

    def one_block(first_row):
        return attend(query_all, key_segment, key_all, value_all, key_segment)

    results = lax.map(one_block, jnp.arange(slot_count // block_rows, dtype=jnp.int32) * block_rows)
    returning = results.reshape(devices, bucket_rows, head_cols)
    returned = lax.all_to_all(returning, "seq", split_axis=0, concat_axis=0, tiled=True)
    returned = returned.reshape(groups, slices * bucket_rows, head_cols)
    attention = (
        jnp.take(returned, slot_place, axis=1).transpose(1, 0, 2).reshape(tok_rows, width_all)
    )
    gate_rows = jnp.take(gate_table.reshape(requests * 2, width_all), segment * 2 + stream, axis=0)
    mixed = hidden.astype(jnp.float32) + gate_rows.astype(jnp.float32) * attention.astype(
        jnp.float32
    )
    return mixed.astype(jnp.bfloat16)


LANES = 128
CONTRACT_LAST = (((1,), (1,)), ((), ()))


def normed(rows, gain_rows):
    wide = rows.astype(jnp.float32)
    inverse = lax.rsqrt(jnp.mean(wide * wide, axis=-1, keepdims=True) + EPSILON)
    return (wide * inverse * gain_rows).astype(jnp.bfloat16)


def fused_kernel(
    devices, requests, segment_hbm, query_hbm, key_hbm, value_hbm,
    text_hbm, hidden_hbm, query_gain_hbm, key_gain_hbm, gate_hbm, out_hbm,
    text_ref, hidden_ref, query_gain_ref, key_gain_ref, gate_ref, out_ref,
    stage, recv, query_n, key_n, result, back, seg_all, hot, text, bias, gate_rows,
    stage_sem, own_sem, seg_own_sem, load_sem, store_sem, seg_send, seg_recv,
    out_send, out_recv, relay_send, relay_recv, back_send, back_recv,
):
    chips = devices // 2
    tok = hidden_hbm.shape[0]
    per_chip = hidden_hbm.shape[1] // HEAD_DIM // chips
    tokens = devices * tok
    mine = chips * tok
    me = lax.axis_index("seq")
    chip, core = me // 2, me % 2
    partner = me + 1 - 2 * core
    sources = (query_hbm, key_hbm, value_hbm)

    def offset(step, of_core):
        return step + of_core * (chips - 2 * step)

    def columns(head):
        return pl.ds(pl.multiple_of(head * HEAD_DIM, HEAD_DIM), HEAD_DIM)

    def remote(src, dst, send_sem, recv_sem, device):
        return pltpu.make_async_remote_copy(
            src_ref=src, dst_ref=dst, send_sem=send_sem, recv_sem=recv_sem,
            device_id={"seq": device}, device_id_type=pl.DeviceIdType.MESH,
        )

    barrier = pltpu.get_barrier_semaphore()
    for device in [(chip + offset(step, core)) % chips * 2 + core for step in range(1, chips)] + [partner]:
        pl.semaphore_signal(
            barrier, inc=1, device_id={"seq": device},
            device_id_type=pl.DeviceIdType.MESH,
        )
    seg_own = pltpu.make_async_copy(segment_hbm, seg_all.at[me], seg_own_sem)
    seg_own.start()
    for head in range(per_chip):
        for step in range(1, chips):
            target = (chip + offset(step, core)) % chips
            for part, source in enumerate(sources):
                pltpu.make_async_copy(
                    source.at[:, columns(target * per_chip + head)],
                    stage.at[head, step - 1, part],
                    stage_sem.at[head],
                ).start()
        for part, source in enumerate(sources):
            pltpu.make_async_copy(
                source.at[:, columns(chip * per_chip + head)],
                recv.at[head, me, part],
                own_sem.at[head],
            ).start()
    loads = [
        pltpu.make_async_copy(source, target, load_sem.at[place])
        for place, (source, target) in enumerate(
            (
                (text_hbm, text_ref), (query_gain_hbm, query_gain_ref),
                (key_gain_hbm, key_gain_ref), (gate_hbm, gate_ref), (hidden_hbm, hidden_ref),
            )
        )
    ]
    for copy in loads:
        copy.start()
    seg_own.wait()
    pl.semaphore_wait(barrier, chips)

    seg_copies = []
    seg_relays = []

    def send_ids(source, kind, step, device):
        copy = remote(
            seg_all.at[source], seg_all.at[source],
            seg_send.at[kind, step], seg_recv.at[kind, step], device,
        )
        copy.start()
        return copy

    for step in range(chips - 1, 0, -1):
        seg_copies.insert(0, send_ids(me, 0, step, (chip + offset(step, core)) % chips * 2 + core))
    seg_relays.append(send_ids(me, 1, 0, partner))
    out_copies = []
    for head in range(per_chip):
        pltpu.make_async_copy(stage.at[head], stage.at[head], stage_sem.at[head]).wait()
        row = []
        for step in range(chips - 1, 0, -1):
            copy = remote(
                stage.at[head, step - 1], recv.at[head, me],
                out_send.at[head, step - 1], out_recv.at[head, step - 1],
                (chip + offset(step, core)) % chips * 2 + core,
            )
            copy.start()
            row.insert(0, copy)
        out_copies.append(row)

    relay_copies = []

    def relay(head, step, source):
        copy = remote(
            recv.at[head, source, pl.ds(1, 2)], recv.at[head, source, pl.ds(1, 2)],
            relay_send.at[head, step], relay_recv.at[head, step], partner,
        )
        copy.start()
        return copy

    for head in range(per_chip):
        pltpu.make_async_copy(
            recv.at[head, me], recv.at[head, me], own_sem.at[head]
        ).wait()
        relay_copies.append([relay(head, 0, me)])

    for step in range(1, chips):
        seg_copies[step - 1].wait_recv()
        source = (chip + chips - offset(step, core)) % chips * 2 + core
        seg_relays.append(send_ids(source, 1, step, partner))
    for copy in seg_relays:
        copy.wait_recv()
    for copy in loads:
        copy.wait()
    eye = (
        lax.broadcasted_iota(jnp.int32, (tok, tok), 0)
        == lax.broadcasted_iota(jnp.int32, (tok, tok), 1)
    ).astype(jnp.float32).astype(jnp.bfloat16)
    ids = lax.broadcasted_iota(jnp.int32, (LANES, tok), 0)
    for n in range(devices):
        flipped = (ids == seg_all[n]).astype(jnp.float32).astype(jnp.bfloat16)
        hot[n] = lax.dot_general(
            eye, flipped, CONTRACT_LAST, preferred_element_type=jnp.float32
        ).astype(jnp.bfloat16)
    all_hot = hot[...].reshape(tokens, LANES)
    earlier = (
        lax.broadcasted_iota(jnp.int32, (tokens, tokens), 1)
        < lax.broadcasted_iota(jnp.int32, (tokens, tokens), 0)
    ).astype(jnp.float32).astype(jnp.bfloat16)
    before = jnp.dot(earlier, all_hot, preferred_element_type=jnp.float32)
    lane = lax.broadcasted_iota(jnp.int32, (1, LANES), 1)
    limit = jnp.zeros((1, LANES), jnp.int32)
    for r in range(requests):
        limit = jnp.where(lane == r, text_ref[0:1, r : r + 1], limit)
    inside = jnp.where(before < limit.astype(jnp.float32), all_hot.astype(jnp.float32), 0.0)
    ones = jnp.ones((LANES, LANES), jnp.bfloat16)
    text[...] = jnp.dot(
        inside.astype(jnp.bfloat16), ones, preferred_element_type=jnp.float32
    ).reshape(devices, tok, LANES)
    for c in range(chips):
        same = lax.dot_general(
            hot[2 * c + core], all_hot, CONTRACT_LAST, preferred_element_type=jnp.float32
        )
        bias[c * tok : (c + 1) * tok] = jnp.where(same > 0.5, 0.0, MASKED)

    number = lax.broadcasted_iota(jnp.int32, (LANES, LANES), 0).astype(jnp.float32)
    own_id = jnp.dot(
        hot[me], number.astype(jnp.bfloat16), preferred_element_type=jnp.float32
    )
    own_code = 2.0 * own_id + jnp.where(text[me] > 0.5, 0.0, 1.0)
    for tile in range(hidden_ref.shape[1] // LANES):
        cols = slice(tile * LANES, (tile + 1) * LANES)
        total = jnp.zeros((tok, LANES), jnp.float32)
        for r in range(requests):
            pair = gate_ref[r, :, cols].astype(jnp.float32)
            for s in range(2):
                total = jnp.where(own_code == float(2 * r + s), pair[s : s + 1], total)
        gate_rows[tile] = total

    query_gain, key_gain = query_gain_ref[...], key_gain_ref[...]

    def gain_of(gain, n):
        return jnp.where(text[n] > 0.5, gain[0:1], gain[1:2])

    scale = 1.0 / math.sqrt(HEAD_DIM)
    back_copies = []
    for head in range(per_chip):
        for step in range(1, chips):
            out_copies[head][step - 1].wait_recv()
            source = (chip + chips - offset(step, core)) % chips * 2 + core
            relay_copies[head].append(relay(head, step, source))
        for c in range(chips):
            n = 2 * c + core
            query_n[c] = normed(recv[head, n, 0], gain_of(query_gain, n))
            key_n[n] = normed(recv[head, n, 1], gain_of(key_gain, n))
        for step in range(chips):
            relay_copies[head][step].wait_recv()
            n = (chip + chips - offset(step, 1 - core)) % chips * 2 + 1 - core
            key_n[n] = normed(recv[head, n, 1], gain_of(key_gain, n))
        keys = key_n[...].reshape(tokens, HEAD_DIM)
        vals = recv[head, :, 2].reshape(tokens, HEAD_DIM)
        scores = lax.dot_general(
            query_n[...].reshape(mine, HEAD_DIM), keys, CONTRACT_LAST,
            preferred_element_type=jnp.float32,
        ) * scale + bias[...]
        largest = jnp.max(scores, axis=-1, keepdims=True)
        weights = jnp.exp(scores - largest)
        weights = (weights / jnp.sum(weights, axis=-1, keepdims=True)).astype(jnp.bfloat16)
        result[head] = jnp.dot(
            weights, vals, preferred_element_type=jnp.float32
        ).astype(jnp.bfloat16).reshape(chips, tok, HEAD_DIM)
        row = []
        for step in range(1, chips):
            target = (chip + offset(step, core)) % chips
            copy = remote(
                result.at[head, target], back.at[chip * per_chip + head],
                back_send.at[head, step - 1], back_recv.at[head, step - 1],
                target * 2 + core,
            )
            copy.start()
            row.append(copy)
        back_copies.append(row)

    def finish(index, attention):
        out_ref[:, columns(index)] = (
            hidden_ref[:, columns(index)].astype(jnp.float32)
            + gate_rows[index] * attention.astype(jnp.float32)
        ).astype(jnp.bfloat16)
        pltpu.make_async_copy(
            out_ref.at[:, columns(index)], out_hbm.at[:, columns(index)], store_sem
        ).start()

    for head in range(per_chip):
        finish(chip * per_chip + head, result[head, chip])
        for step in range(1, chips):
            back_copies[head][step - 1].wait_recv()
            index = (chip + chips - offset(step, core)) % chips * per_chip + head
            finish(index, back[index])
    for copy in seg_copies + seg_relays:
        copy.wait_send()
    for rows in (out_copies, relay_copies, back_copies):
        for row in rows:
            for copy in row:
                copy.wait_send()
    pltpu.make_async_copy(out_ref, out_hbm, store_sem).wait()


def fused(
    hidden, queries, key_rows, values, query_gain, key_gain, gate_table, segment, text_count
):
    devices = lax.axis_size("seq")
    chips = devices // 2
    tok, width = hidden.shape
    heads = width // HEAD_DIM
    per_chip = heads // chips
    hbm = pl.BlockSpec(memory_space=pl.ANY)
    block = (tok, HEAD_DIM)
    dma = pltpu.SemaphoreType.DMA
    return pl.pallas_call(
        functools.partial(fused_kernel, devices, text_count.shape[0]),
        out_shape=jax.ShapeDtypeStruct((tok, width), jnp.bfloat16),
        in_specs=[hbm] * 9,
        out_specs=hbm,
        scratch_shapes=[
            pltpu.VMEM((1, text_count.shape[0]), jnp.int32),
            pltpu.VMEM(hidden.shape, hidden.dtype),
            pltpu.VMEM(query_gain.shape, query_gain.dtype),
            pltpu.VMEM(key_gain.shape, key_gain.dtype),
            pltpu.VMEM(gate_table.shape, gate_table.dtype),
            pltpu.VMEM(hidden.shape, jnp.bfloat16),
            pltpu.VMEM((per_chip, chips - 1, 3) + block, jnp.bfloat16),
            pltpu.VMEM((per_chip, devices, 3) + block, jnp.bfloat16),
            pltpu.VMEM((chips,) + block, jnp.bfloat16),
            pltpu.VMEM((devices,) + block, jnp.bfloat16),
            pltpu.VMEM((per_chip, chips) + block, jnp.bfloat16),
            pltpu.VMEM((heads,) + block, jnp.bfloat16),
            pltpu.VMEM((devices, 1, tok), jnp.int32),
            pltpu.VMEM((devices, tok, LANES), jnp.bfloat16),
            pltpu.VMEM((devices, tok, LANES), jnp.float32),
            pltpu.VMEM((chips * tok, devices * tok), jnp.float32),
            pltpu.VMEM((heads, tok, LANES), jnp.float32),
            dma((per_chip,)),
            dma((per_chip,)),
            dma,
            dma((5,)),
            dma,
            dma((2, chips)),
            dma((2, chips)),
            dma((per_chip, chips - 1)),
            dma((per_chip, chips - 1)),
            dma((per_chip, chips)),
            dma((per_chip, chips)),
            dma((per_chip, chips - 1)),
            dma((per_chip, chips - 1)),
        ],
        compiler_params=pltpu.CompilerParams(collective_id=0, has_side_effects=True),
    )(
        segment.reshape(1, tok), queries, key_rows, values,
        text_count.reshape(1, -1), hidden, query_gain, key_gain, gate_table,
    )


def program(*arrays):
    devices = lax.axis_size("seq")
    tok, width = arrays[0].shape
    requests = arrays[-1].shape[0]
    whole_heads = devices % 2 == 0 and (width // HEAD_DIM) % (devices // 2) == 0
    if whole_heads and devices * tok <= 1024 and requests <= LANES and tok % 16 == 0:
        return fused(*arrays)
    return per_device(*arrays)


def solution(mesh):
    return jax.shard_map(
        program,
        mesh=mesh,
        in_specs=(
            P(("groups", "seq"), None),
            P(("groups", "seq"), None),
            P(("groups", "seq"), None),
            P(("groups", "seq"), None),
            P(),
            P(),
            P("groups", None, None),
            P(("groups", "seq")),
            P("groups"),
        ),
        out_specs=P(("groups", "seq"), None),
        check_vma=False,
    )
```
